32 devices in a mesh: seq: 8 (over z, y), mp: 4 (over x, core).
Axes of the slice: x: 2, y: 2, z: 4, core: 2. Of those that a mesh axis runs over, the one named last changes fastest.
Arguments:
- gate_in: bfloat16 [8192, 1024], P('seq', 'mp'), may hold values from -5 to 5
- value_in: bfloat16 [8192, 1024], P('seq', 'mp'), may hold values from -5 to 5
- out_gate: bfloat16 [8192, 1024], P('seq', 'mp'), may hold values from -10 to 10
- filter_taps: bfloat16 [4096, 1024], P('seq', 'mp'), may hold values from -0.09375 to 0.09375
- skip_gain: float32 [1024], P('mp'), may hold values from -4 to 4
Outputs:
- output: bfloat16 [8192, 1024], P('seq', 'mp')
The draws below stay inside these ranges and needn't reach their ends.
All inputs are finite; a program needn't handle non-finite values.
Results may differ from the reference program's by a relative error of at most 0.009.
Values may be sent and summed in bfloat16 or wider, within the bound.
No kernel may reach another device: no remote copies, remote signals or barrier semaphores. Data moves between devices by JAX's collectives and lax.ppermute only.
A program may use at most 64 MiB of HBM per device.

```python
import math
import jax
import jax.numpy as jnp
from jax import lax

C = 1024
K = 4096
TOKENS = 8192


def draw_out_gate(key, part):
    first_key, second_key = jax.random.split(jax.random.fold_in(key, 11), 2)
    position = jnp.arange(C, dtype=jnp.float32) / (C - 1)
    ramp = 0.55 * jnp.power(3.0, position)
    channel_scale = jnp.exp(jax.random.uniform(second_key, (C,), jnp.float32, math.log(0.7), math.log(1.4)))
    base = jnp.clip(jax.random.normal(first_key, (TOKENS, C), jnp.float32), -4.0, 4.0)
    return (base * ramp[None, :] * channel_scale[None, :]).astype(jnp.bfloat16)


def block_scale(key, dims, pieces, smallest, largest):
    def one(dim, parts):
        draws = jax.random.uniform(jax.random.fold_in(jax.random.fold_in(key, 6), dim), (parts,), jnp.float32, smallest / len(pieces), largest / len(pieces))
        return jnp.repeat(jnp.exp(draws), dims[dim] // parts).reshape((-1,) + (1,) * (len(dims) - dim - 1))

    loudness = one(*pieces[0])
    for cut in pieces[1:]:
        loudness = loudness * one(*cut)
    return loudness


def gaussian(stream_key, extent, scale, bound, cuts=(), held_as=jnp.bfloat16):
    loudness = block_scale(stream_key, extent, cuts, -0.22, 0.18) if cuts else 1.0
    entries = jax.random.normal(stream_key, extent, jnp.float32) * scale * loudness
    return jnp.minimum(jnp.maximum(entries, -bound), bound).astype(held_as)


def setup_inputs(seed: int = 0) -> dict:
    keys = jax.random.split(jax.random.key(seed), 6)
    return {
        "gate_in": gaussian(keys[0], (TOKENS, C), 1.0, 5.0, ((0, 8), (1, 4))),
        "value_in": gaussian(keys[1], (TOKENS, C), 1.0, 5.0, ((0, 8), (1, 4))),
        "out_gate": draw_out_gate(jax.random.fold_in(keys[5], 71), 0),
        "filter_taps": gaussian(keys[3], (K, C), K ** -0.5, 0.09375, ((0, 8), (1, 4))),
        "skip_gain": gaussian(keys[4], (C,), 1.0, 4.0, ((0, 4),), jnp.float32),
    }


def convolve_group(signal_kernel):
    signal, kernel = signal_kernel
    length = signal.shape[1]
    size = 1 << (length + kernel.shape[1] - 1).bit_length()
    product = jnp.fft.rfft(signal, size) * jnp.fft.rfft(kernel, size)
    return jnp.fft.irfft(product, size)[:, :length]

def reference(gate_in, value_in, out_gate, filter_taps, skip_gain):
    gated = (gate_in.astype(jnp.float32) * value_in.astype(jnp.float32)).astype(jnp.bfloat16)
    group = 32
    signal = gated.astype(jnp.float32).T.reshape(C // group, group, TOKENS)
    kernel = filter_taps.astype(jnp.float32).T.reshape(C // group, group, K)
    convolved = lax.map(convolve_group, (signal, kernel)).reshape(C, TOKENS).T
    mixed = out_gate.astype(jnp.float32) * (convolved + skip_gain[None, :] * gated.astype(jnp.float32))
    power = lax.optimization_barrier(jnp.mean(mixed * mixed, axis=1, keepdims=True))
    return (mixed / jnp.sqrt(power + 1e-05)).astype(jnp.bfloat16)
```

```python
import functools

import jax
import jax.numpy as jnp
from jax import lax
from jax.experimental import pallas as pl
from jax.experimental.pallas import tpu as pltpu
from jax.sharding import PartitionSpec as P

LANES = 128
HALF = LANES // 2
WIDE = 2 * LANES
BF16 = jnp.bfloat16
F32 = jnp.float32
NT = (((1,), (1,)), ((), ()))


def vmem_call(body, out_shape, scratch=(), flops=0, name=None):
    return pl.pallas_call(
        body,
        out_shape=out_shape,
        scratch_shapes=list(scratch),
        cost_estimate=pl.CostEstimate(flops=flops, bytes_accessed=0, transcendentals=0),
        name=name,
    )


def unit_matrix(size):
    row = lax.broadcasted_iota(jnp.int32, (size, size), 0)
    column = lax.broadcasted_iota(jnp.int32, (size, size), 1)
    return jnp.where(row == column, 1.0, 0.0).astype(BF16)


def flip(matrix, unit):
    return lax.dot_general(unit, matrix, NT, preferred_element_type=F32).astype(BF16)


def prepare(gate_ref, value_ref, taps_ref, og_ref, gated_ref, taps_out_ref, og_out_ref):
    channels = gate_ref.shape[1]
    unit = unit_matrix(channels)
    step = min(WIDE, gate_ref.shape[0])
    for start in range(0, gate_ref.shape[0], step):
        rows = pl.ds(start, step)
        gated = (gate_ref[rows, :].astype(F32) * value_ref[rows, :].astype(F32)).astype(BF16)
        gated_ref[:, rows] = flip(gated, unit)
        og_out_ref[:, rows] = flip(og_ref[rows, :], unit)
    taps_out_ref[...] = flip(taps_ref[...], unit)


def conv_body(x_ref, h_ref, y_ref, xs, hs, xp, xr, lhs, rhs, s1, s2, ys):
    sources, channels, span = x_ref.shape
    per_source = span // LANES
    blocks = sources * per_source
    h_sources, _, h_span = h_ref.shape
    h_per = h_span // LANES
    h_blocks = h_sources * h_per
    pieces = lhs.shape[1] // LANES
    pad = xp.shape[0] - blocks
    for s in range(sources):
        for b in range(per_source):
            at = (s * per_source + b) * channels
            xs[pl.ds(at, channels), :] = x_ref[s, :, pl.ds(b * LANES, LANES)].astype(F32)
    for s in range(h_sources):
        for b in range(h_per):
            at = (s * h_per + b) * channels
            hs[pl.ds(at, channels), :] = h_ref[s, :, pl.ds(b * LANES, LANES)].astype(F32)
    xp[pl.ds(0, pad), :] = jnp.zeros((pad, LANES), F32)
    xr[pl.ds(0, pad), :] = jnp.zeros((pad, LANES), F32)
    s1[pl.ds(0, 8), :] = jnp.zeros((8, LANES), F32)
    s2[pl.ds(0, 8), :] = jnp.zeros((8, LANES), F32)
    rhs[pl.ds(h_blocks * HALF // 2, LANES), :] = jnp.zeros((LANES, WIDE), BF16)
    lane = lax.broadcasted_iota(jnp.int32, (HALF, LANES), 1)
    row = lax.broadcasted_iota(jnp.int32, (HALF, LANES), 0)
    ahead = lane >= row
    low = lax.broadcasted_iota(jnp.int32, (blocks, LANES), 1) < HALF

    def channel(c, carry):
        before = jnp.zeros((HALF, LANES), F32)
        for m in range(h_blocks + 1):
            if m < h_blocks:
                line = jnp.broadcast_to(hs[pl.ds(m * channels + c, 1), :], (HALF, LANES))
                now = pltpu.roll(line, 0, 1, stride=1, stride_axis=0)
            else:
                now = jnp.zeros((HALF, LANES), F32)
            tile = jnp.where(ahead, now, before).astype(BF16)
            rhs[pl.ds((m // 2) * HALF, HALF), pl.ds((m % 2) * LANES, LANES)] = tile
            before = now
        x = xs[pl.ds(c, blocks, stride=channels), :]
        xp[pl.ds(pad, blocks), :] = x
        xr[pl.ds(pad, blocks), :] = pltpu.roll(x, HALF, 1)
        for p in range(pieces):
            near = pl.ds(pad - 4 * p, blocks)
            far = pl.ds(pad - 4 * p - 2, blocks)
            at = pl.ds(p * LANES, LANES)
            lhs[pl.ds(0, blocks), at] = jnp.where(low, xp[near, :], xr[far, :]).astype(BF16)
            lhs[pl.ds(blocks, blocks), at] = jnp.where(low, xr[near, :], xp[far, :]).astype(BF16)
        z = jnp.dot(lhs[...], rhs[...], preferred_element_type=F32)
        first = pltpu.roll(z[blocks:, :LANES], HALF, 1)
        second = pltpu.roll(z[blocks:, LANES:], HALF, 1)
        s1[pl.ds(8, blocks), :] = z[:blocks, LANES:] + jnp.where(low, first, second)
        s2[pl.ds(8, blocks), :] = jnp.where(low, second, 0.0)
        y = z[:blocks, :LANES] + jnp.where(low, 0.0, first)
        y = y + s1[pl.ds(7, blocks), :] + s2[pl.ds(6, blocks), :]
        ys[pl.ds(c, blocks, stride=channels), :] = y
        return carry

    lax.fori_loop(0, channels, channel, 0)
    for s in range(sources):
        for b in range(per_source):
            at = (s * per_source + b) * channels
            y_ref[s, :, pl.ds(b * LANES, LANES)] = ys[pl.ds(at, channels), :].astype(BF16)


def convolve(x, h):
    sources, channels, span = x.shape
    if h.shape[2] % LANES:
        h = jnp.moveaxis(h, 0, 1).reshape(1, channels, -1)
    blocks = sources * span // LANES
    taps = h.shape[0] * h.shape[2]
    h_blocks = taps // LANES
    deep = h_blocks * HALF // 2 * 1 + LANES
    pieces = deep // LANES
    pad = -(-(4 * pieces) // 8) * 8
    scratch = [
        pltpu.VMEM((blocks * channels, LANES), F32),
        pltpu.VMEM((h_blocks * channels, LANES), F32),
        pltpu.VMEM((pad + blocks, LANES), F32),
        pltpu.VMEM((pad + blocks, LANES), F32),
        pltpu.VMEM((2 * blocks, deep), BF16),
        pltpu.VMEM((deep, WIDE), BF16),
        pltpu.VMEM((8 + blocks, LANES), F32),
        pltpu.VMEM((8 + blocks, LANES), F32),
        pltpu.VMEM((blocks * channels, LANES), F32),
    ]
    return vmem_call(
        conv_body,
        jax.ShapeDtypeStruct(x.shape, BF16),
        scratch,
        flops=2 * channels * 2 * blocks * deep * WIDE,
        name="conv",
    )(x, h)


def mix(conv_ref, gated_ref, og_ref, skip_ref, mixed_ref, power_ref):
    mixed = og_ref[...].astype(F32) * (
        conv_ref[...].astype(F32) + skip_ref[...] * gated_ref[...].astype(F32)
    )
    mixed_ref[...] = mixed
    power_ref[...] = jnp.sum(mixed * mixed, axis=0, keepdims=True)


def finish(total, mixed_ref, power_ref, out_ref):
    scale = 1.0 / jnp.sqrt(power_ref[...] / total + 1e-05)
    step = min(WIDE, out_ref.shape[0])
    unit = unit_matrix(step)
    for start in range(0, out_ref.shape[0], step):
        rows = pl.ds(start, step)
        out_ref[rows, :] = flip((mixed_ref[:, rows] * scale[:, start : start + step]).astype(BF16), unit)


def spread_sum(value, axis, size):
    total = value
    for d in range(1, size):
        total = total + lax.ppermute(value, axis, [(j, (j + d) % size) for j in range(size)])
    return total


def local(n_seq, n_mp, gate_in, value_in, out_gate, filter_taps, skip_gain):
    tokens, channels = gate_in.shape
    taps = filter_taps.shape[0]
    share = channels // n_seq
    gated, taps_t, og = vmem_call(
        prepare,
        (
            jax.ShapeDtypeStruct((channels, tokens), BF16),
            jax.ShapeDtypeStruct((channels, taps), BF16),
            jax.ShapeDtypeStruct((channels, tokens), BF16),
        ),
        name="prepare",
        flops=4 * channels * channels * tokens,
    )(gate_in, value_in, filter_taps, out_gate)
    swap = functools.partial(lax.all_to_all, axis_name="seq", split_axis=0, concat_axis=0, tiled=True)
    h = swap(taps_t.reshape(n_seq, share, taps))
    x = swap(gated.reshape(n_seq, share, tokens))
    y = swap(convolve(x, h)).reshape(channels, tokens)
    mixed, power = vmem_call(
        mix,
        (
            jax.ShapeDtypeStruct((channels, tokens), F32),
            jax.ShapeDtypeStruct((1, tokens), F32),
        ),
        name="mix",
        flops=8 * channels * tokens,
    )(y, gated, og, skip_gain.reshape(channels, 1))
    power = spread_sum(power, "mp", n_mp)
    return vmem_call(
        functools.partial(finish, channels * n_mp),
        jax.ShapeDtypeStruct((tokens, channels), BF16),
        name="finish",
        flops=4 * channels * tokens * WIDE,
    )(mixed, power)


def solution(mesh):
    return jax.shard_map(
        functools.partial(local, mesh.shape["seq"], mesh.shape["mp"]),
        mesh=mesh,
        in_specs=(P("seq", "mp"), P("seq", "mp"), P("seq", "mp"), P("seq", "mp"), P("mp")),
        out_specs=P("seq", "mp"),
        check_vma=False,
    )
```

```python
import functools

import jax
import jax.numpy as jnp
from jax import lax
from jax.experimental import pallas as pl
from jax.experimental.pallas import tpu as pltpu
from jax.sharding import PartitionSpec as P

LANES = 128
HALF = LANES // 2
WIDE = 2 * LANES
CHUNKS = 1
BF16 = jnp.bfloat16
F32 = jnp.float32
NT = (((1,), (1,)), ((), ()))


def vmem_call(body, out_shape, scratch=(), flops=0, name=None, limit=6, inputs=1):
    spec = pl.BlockSpec(memory_space=pltpu.VMEM)
    return pl.pallas_call(
        body,
        out_shape=out_shape,
        in_specs=[spec] * inputs,
        out_specs=[spec] * len(out_shape) if isinstance(out_shape, (list, tuple)) else spec,
        scratch_shapes=list(scratch),
        compiler_params=pltpu.CompilerParams(vmem_limit_bytes=limit << 20),
        cost_estimate=pl.CostEstimate(flops=flops, bytes_accessed=0, transcendentals=0),
        name=name,
    )


def unit_matrix(size):
    row = lax.broadcasted_iota(jnp.int32, (size, size), 0)
    column = lax.broadcasted_iota(jnp.int32, (size, size), 1)
    return jnp.where(row == column, 1.0, 0.0).astype(BF16)


def flip(matrix, unit):
    return lax.dot_general(unit, matrix, NT, preferred_element_type=F32).astype(BF16)


def deal(flipped, refs, span):
    owners, part, _ = refs[0].shape
    for owner in range(owners):
        for k, ref in enumerate(refs):
            at = (owner * len(refs) + k) * part
            ref[owner, :, span] = flipped[at : at + part, :]


def flip_in(gate_ref, value_ref, taps_ref, *out_refs):
    unit = unit_matrix(gate_ref.shape[1])
    tokens = gate_ref.shape[0]
    step = min(WIDE, tokens)

    def some(i, carry):
        rows = pl.ds(pl.multiple_of(i * step, step), step)
        gated = (gate_ref[rows, :].astype(F32) * value_ref[rows, :].astype(F32)).astype(BF16)
        deal(flip(gated, unit), out_refs, rows)
        return carry

    lax.fori_loop(0, tokens // step, some, 0)
    deal(flip(taps_ref[...], unit), out_refs, pl.ds(tokens, taps_ref.shape[0]))


def flip_out_gate(og_ref, skip_ref, column_ref, *out_refs):
    unit = unit_matrix(og_ref.shape[1])
    step = min(WIDE, og_ref.shape[0])

    def some(i, carry):
        rows = pl.ds(pl.multiple_of(i * step, step), step)
        deal(flip(og_ref[rows, :], unit), out_refs, rows)
        return carry

    lax.fori_loop(0, og_ref.shape[0] // step, some, 0)
    column_ref[...] = jnp.broadcast_to(skip_ref[...], (LANES, skip_ref.shape[1])).T


UNROLL = 2
PACK = 16

def conv_body(*refs):
    x_ref, h_ref = refs[0], refs[-6]
    y_ref, vs, hs, zs0, zs1 = refs[-5:]
    sources, channels, span = y_ref.shape
    per_source = span // LANES
    blocks = sources * per_source
    h_sources = h_ref.shape[0]
    h_from = span if h_ref is x_ref else 0
    h_per = (h_ref.shape[2] - h_from) // LANES
    h_blocks = h_sources * h_per
    rows = 2 * blocks
    pitch = channels + 8
    low = lax.broadcasted_iota(jnp.int32, (channels, LANES), 1) < HALF
    zero = jnp.zeros((channels, LANES), F32)

    def place(s, b, j):
        at = (8 * (per_source * s // 4 + b // 4) + 4 * j + b % 4) * pitch
        return pl.ds(at if pitch % 8 else pl.multiple_of(at, 8), channels)

    def spread(s, carry):
        older, old = carry
        for b in range(per_source):
            x = x_ref[s, :, pl.ds(b * LANES, LANES)].astype(F32)
            turned = pltpu.roll(x, HALF, 1)
            vs[place(s, b, 0), :] = jnp.where(low, x, older[1])
            vs[place(s, b, 1), :] = jnp.where(low, turned, older[0])
            older, old = old, (x, turned)
        return older, old

    lax.fori_loop(0, sources, spread, ((zero, zero), (zero, zero)))

    def spread_taps(s, carry):
        for b in range(h_per):
            at = (s * h_per + b) * pitch
            at = at if pitch % 8 else pl.multiple_of(at, 8)
            hs[pl.ds(at, channels), :] = h_ref[s, :, pl.ds(h_from + b * LANES, LANES)].astype(F32)
        return carry

    lax.fori_loop(0, h_sources, spread_taps, 0)

    lane = lax.broadcasted_iota(jnp.int32, (PACK, LANES), 1)
    row = lax.broadcasted_iota(jnp.int32, (PACK, LANES), 0)
    ahead = lane >= row
    lane16 = lane.astype(F32).astype(BF16)

    def channel(c):
        v = vs[pl.ds(c, rows, stride=pitch), :]
        even = v.astype(BF16)
        odd = jnp.concatenate([jnp.zeros((8, LANES), F32), v[:-8]], axis=0).astype(BF16)
        before = jnp.zeros((PACK, LANES), F32)
        turns = [jnp.zeros((PACK, LANES), BF16)] * (HALF // PACK)
        tiles = []
        z = None
        for m in range(h_blocks + 1):
            if m < h_blocks:
                line = jnp.broadcast_to(hs[pl.ds(m * pitch + c, 1), :], (PACK, LANES))
                now = pltpu.roll(line, 0, 1, stride=1, stride_axis=0)
            else:
                now = jnp.zeros((PACK, LANES), F32)
            base = jnp.where(ahead, now, before).astype(BF16)
            before = now
            group = [base]
            for q in range(1, HALF // PACK):
                turned = pltpu.roll(base, PACK * q, 1)
                group.append(jnp.where(lane16 >= PACK * q, turned, turns[q]))
                turns[q] = turned
            tiles.append(jnp.concatenate(group, axis=0))
            if m % 8 == 7 or m == h_blocks:
                k = m // 8
                top = PACK * k
                left = rows - top
                if m < h_blocks:
                    weight = jnp.concatenate(
                        [jnp.concatenate(tiles[i : i + 2], axis=1) for i in range(0, 8, 2)], axis=0
                    )
                    data = jnp.concatenate([even[:left], odd[:left]], axis=1)
                else:
                    weight = jnp.concatenate([tiles[0], jnp.zeros((HALF, LANES), BF16)], axis=0)
                    weight = jnp.concatenate([weight, jnp.zeros((LANES, LANES), BF16)], axis=1)
                    data = even[:left]
                part = jnp.dot(data, weight, preferred_element_type=F32)
                z = part if z is None else jnp.concatenate([z[:top], z[top:] + part], axis=0)
                tiles = []
        zs0[pl.ds(c, rows, stride=pitch), :] = z[:, :LANES]
        zs1[pl.ds(c, rows, stride=pitch), :] = z[:, LANES:]

    def group(g, carry):
        for i in range(UNROLL):
            channel(g * UNROLL + i)
        return carry

    lax.fori_loop(0, channels // UNROLL, group, 0)

    def gather(s, carry):
        late1, late2, late22 = carry
        for b in range(per_source):
            first = pltpu.roll(zs0[place(s, b, 1), :], HALF, 1)
            second = pltpu.roll(zs1[place(s, b, 1), :], HALF, 1)
            y = zs0[place(s, b, 0), :] + jnp.where(low, 0.0, first) + late1 + late22
            late1 = zs1[place(s, b, 0), :] + jnp.where(low, first, second)
            late22, late2 = late2, jnp.where(low, second, 0.0)
            y_ref[s, :, pl.ds(b * LANES, LANES)] = y.astype(BF16)
        return late1, late2, late22

    lax.fori_loop(0, sources, gather, (zero, zero, zero))


def convolve(data, span):
    sources, channels, both = data.shape
    taps = sources * (both - span)
    inputs = [data]
    if (both - span) % LANES:
        inputs.append(jnp.moveaxis(data[:, :, span:], 0, 1).reshape(1, channels, taps))
    blocks = sources * span // LANES
    scratch = [
        pltpu.VMEM((2 * blocks * (channels + 8), LANES), F32),
        pltpu.VMEM((taps // LANES * (channels + 8), LANES), F32),
        pltpu.VMEM((2 * blocks * (channels + 8), LANES), F32),
        pltpu.VMEM((2 * blocks * (channels + 8), LANES), F32),
    ]
    return vmem_call(
        conv_body,
        jax.ShapeDtypeStruct((sources, channels, span), BF16),
        scratch,
        flops=4 * channels * blocks * (taps // 4 + HALF) * WIDE,
        name="conv",
        limit=28,
        inputs=len(inputs),
    )(*inputs)


def mix(k, chunks, has_before, y_ref, gated_ref, og_ref, column_ref, *refs):
    mixed_ref, power_ref = refs[-2:]
    owners, part, tokens = y_ref.shape
    power_ref[...] = refs[0][...] if has_before else jnp.zeros((8, tokens), F32)

    def some(owner, carry):
        at = (owner * chunks + k) * part
        skip = column_ref[pl.ds(at if part % 8 else pl.multiple_of(at, 8), part), :1]
        mixed = og_ref[owner].astype(F32) * (
            y_ref[owner].astype(F32) + skip * gated_ref[owner, :, :tokens].astype(F32)
        )
        mixed_ref[owner] = mixed
        square = mixed * mixed
        if part % 8:
            power_ref[pl.ds(0, 1), :] += jnp.sum(square, axis=0, keepdims=True)
        else:
            power_ref[...] += jnp.sum(square.reshape(part // 8, 8, tokens), axis=0)
        return carry

    lax.fori_loop(0, owners, some, 0)
    power_ref[...] = jnp.broadcast_to(jnp.sum(power_ref[...], axis=0, keepdims=True), (8, tokens))


def finish(total, peers, *refs):
    powers, mixed, out_ref = refs[:peers], refs[peers:-1], refs[-1]
    step = min(WIDE, out_ref.shape[0])
    unit = unit_matrix(step)
    owners = mixed[0].shape[0]

    def some(i, carry):
        rows = pl.ds(pl.multiple_of(i * step, step), step)
        power = powers[0][:1, rows]
        for other in powers[1:]:
            power = power + other[:1, rows]
        scale = 1.0 / jnp.sqrt(power / total + 1e-05)
        pieces = [
            (ref[owner, :, rows] * scale).astype(BF16) for owner in range(owners) for ref in mixed
        ]
        out_ref[rows, :] = flip(jnp.concatenate(pieces, axis=0), unit)
        return carry

    lax.fori_loop(0, out_ref.shape[0] // step, some, 0)


def local(n_seq, n_mp, gate_in, value_in, out_gate, filter_taps, skip_gain):
    tokens, channels = gate_in.shape
    taps = filter_taps.shape[0]
    share = channels // n_seq
    chunks = CHUNKS if share % (16 * CHUNKS) == 0 else 1
    part = share // chunks
    swap = functools.partial(lax.all_to_all, axis_name="seq", split_axis=0, concat_axis=0, tiled=True)
    dealt = [jax.ShapeDtypeStruct((n_seq, part, tokens), BF16)] * chunks
    dealt_both = [jax.ShapeDtypeStruct((n_seq, part, tokens + taps), BF16)] * chunks
    column = jax.ShapeDtypeStruct((channels, LANES), F32)
    flat = [jax.ShapeDtypeStruct((n_seq, part, tokens), F32), jax.ShapeDtypeStruct((8, tokens), F32)]
    product = 2 * channels * channels
    both = vmem_call(
        flip_in, dealt_both, name="flip_in", flops=product * (tokens + taps), inputs=3
    )(gate_in, value_in, filter_taps)
    moved = [swap(piece) for piece in both]
    skip, *og = vmem_call(
        flip_out_gate, [column] + dealt, name="flip_out_gate", flops=product * tokens, inputs=2
    )(out_gate, skip_gain.reshape(1, channels))
    y = [swap(convolve(piece, tokens)) for piece in moved]
    mixed, power = [], None
    for k in range(chunks):
        before = [] if power is None else [power]
        piece, power = vmem_call(
            functools.partial(mix, k, chunks, bool(before)),
            flat,
            name="mix",
            flops=8 * channels * tokens,
            inputs=4 + len(before),
        )(y[k], both[k], og[k], skip, *before)
        mixed.append(piece)
    powers = [power] + [
        lax.ppermute(power[:1], "mp", [(j, (j + d) % n_mp) for j in range(n_mp)])
        for d in range(1, n_mp)
    ]
    return vmem_call(
        functools.partial(finish, channels * n_mp, n_mp),
        jax.ShapeDtypeStruct((tokens, channels), BF16),
        name="finish",
        flops=2 * channels * tokens * WIDE,
        inputs=n_mp + chunks,
    )(*powers, *mixed)


def solution(mesh):
    return jax.shard_map(
        functools.partial(local, mesh.shape["seq"], mesh.shape["mp"]),
        mesh=mesh,
        in_specs=(P("seq", "mp"), P("seq", "mp"), P("seq", "mp"), P("seq", "mp"), P("mp")),
        out_specs=P("seq", "mp"),
        check_vma=False,
    )
```

```python
import functools
import math

import jax
import jax.numpy as jnp
from jax import lax
from jax.experimental import pallas as pl
from jax.experimental.pallas import tpu as pltpu
from jax.sharding import PartitionSpec as P

LANES = 128
HALF = LANES // 2
WIDE = 2 * LANES
CHUNKS = 1
BF16 = jnp.bfloat16
F32 = jnp.float32
NT = (((1,), (1,)), ((), ()))


def vmem_call(
    body, out_shape, scratch=(), flops=0, name=None, limit=6, inputs=1, fetch=False, store=False
):
    spec, placed = pl.BlockSpec(memory_space=pltpu.VMEM), pl.BlockSpec(memory_space=pltpu.HBM)
    out_spec = placed if store else spec
    return pl.pallas_call(
        body,
        out_shape=out_shape,
        in_specs=[placed if fetch else spec] * inputs,
        out_specs=[out_spec] * len(out_shape) if isinstance(out_shape, (list, tuple)) else out_spec,
        scratch_shapes=list(scratch),
        compiler_params=pltpu.CompilerParams(vmem_limit_bytes=limit << 20),
        cost_estimate=pl.CostEstimate(flops=flops, bytes_accessed=0, transcendentals=0),
        name=name,
    )


def unit_matrix(size):
    row = lax.broadcasted_iota(jnp.int32, (size, size), 0)
    column = lax.broadcasted_iota(jnp.int32, (size, size), 1)
    return jnp.where(row == column, 1.0, 0.0).astype(BF16)


def flip(matrix, unit):
    return lax.dot_general(unit, matrix, NT, preferred_element_type=F32).astype(BF16)


def deal(flipped, refs, span):
    owners, part, _ = refs[0].shape
    for owner in range(owners):
        for k, ref in enumerate(refs):
            at = (owner * len(refs) + k) * part
            ref[owner, :, span] = flipped[at : at + part, :]


def flip_in(gate_hbm, value_hbm, taps_hbm, *refs):
    out_refs, (gate_ref, value_ref, taps_ref, sems) = refs[:-4], refs[-4:]
    tokens = gate_ref.shape[0]
    step = min(WIDE, tokens)
    steps = tokens // step

    def arrive(source, target, lane, i):
        rows = pl.ds(i * step if isinstance(i, int) else pl.multiple_of(i * step, step), step)
        return pltpu.make_async_copy(source.at[rows, :], target.at[rows, :], sems.at[lane, i])

    for i in range(steps):
        arrive(gate_hbm, gate_ref, 0, i).start()
        arrive(value_hbm, value_ref, 1, i).start()
    rest = pltpu.make_async_copy(taps_hbm, taps_ref, sems.at[2, 0])
    rest.start()
    unit = unit_matrix(gate_ref.shape[1])

    def some(i, carry):
        rows = pl.ds(pl.multiple_of(i * step, step), step)
        arrive(gate_hbm, gate_ref, 0, i).wait()
        arrive(value_hbm, value_ref, 1, i).wait()
        gated = (gate_ref[rows, :].astype(F32) * value_ref[rows, :].astype(F32)).astype(BF16)
        deal(flip(gated, unit), out_refs, rows)
        return carry

    lax.fori_loop(0, steps, some, 0)
    rest.wait()
    deal(flip(taps_ref[...], unit), out_refs, pl.ds(tokens, taps_ref.shape[0]))


def flip_out_gate(og_ref, skip_ref, column_ref, *out_refs):
    unit = unit_matrix(og_ref.shape[1])
    step = min(WIDE, og_ref.shape[0])

    def some(i, carry):
        rows = pl.ds(pl.multiple_of(i * step, step), step)
        deal(flip(og_ref[rows, :], unit), out_refs, rows)
        return carry

    lax.fori_loop(0, og_ref.shape[0] // step, some, 0)
    column_ref[...] = jnp.broadcast_to(skip_ref[...], (LANES, skip_ref.shape[1])).T


UNROLL = 8
PACK = 16

def conv_body(*refs):
    x_ref, h_ref = refs[0], refs[-6]
    y_ref, vs, hs, zs0, zs1 = refs[-5:]
    sources, channels, span = y_ref.shape
    per_source = span // LANES
    blocks = sources * per_source
    h_sources = h_ref.shape[0]
    h_from = span if h_ref is x_ref else 0
    h_per = (h_ref.shape[2] - h_from) // LANES
    h_blocks = h_sources * h_per
    rows = 2 * blocks
    pitch = channels + 8
    each = math.gcd(UNROLL, channels)
    low = lax.broadcasted_iota(jnp.int32, (channels, LANES), 1) < HALF
    zero = jnp.zeros((channels, LANES), F32)

    def place(s, b, j):
        at = (8 * (per_source * s // 4 + b // 4) + 4 * j + b % 4) * pitch
        return pl.ds(at if pitch % 8 else pl.multiple_of(at, 8), channels)

    def spread(s, carry):
        older, old = carry
        for b in range(per_source):
            x = x_ref[s, :, pl.ds(b * LANES, LANES)].astype(F32)
            turned = pltpu.roll(x, HALF, 1)
            vs[place(s, b, 0), :] = jnp.where(low, x, older[1])
            vs[place(s, b, 1), :] = jnp.where(low, turned, older[0])
            older, old = old, (x, turned)
        return older, old

    lax.fori_loop(0, sources, spread, ((zero, zero), (zero, zero)))

    def spread_taps(s, carry):
        for b in range(h_per):
            at = (s * h_per + b) * pitch
            at = at if pitch % 8 else pl.multiple_of(at, 8)
            hs[pl.ds(at, channels), :] = h_ref[s, :, pl.ds(h_from + b * LANES, LANES)].astype(F32)
        return carry

    lax.fori_loop(0, h_sources, spread_taps, 0)

    lane = lax.broadcasted_iota(jnp.int32, (HALF, LANES), 1)
    row = lax.broadcasted_iota(jnp.int32, (HALF, LANES), 0)
    ahead = lane >= row

    def channel(c):
        v = vs[pl.ds(c, rows, stride=pitch), :]
        even = v.astype(BF16)
        odd = jnp.concatenate([jnp.zeros((8, LANES), F32), v[:-8]], axis=0).astype(BF16)
        before = jnp.zeros((HALF, LANES), F32)
        tiles = []
        z = None
        for m in range(h_blocks + 1):
            if m < h_blocks:
                line = jnp.broadcast_to(hs[pl.ds(m * pitch + c, 1), :], (HALF, LANES))
                now = pltpu.roll(line, 0, 1, stride=1, stride_axis=0)
            else:
                now = jnp.zeros((HALF, LANES), F32)
            tiles.append(jnp.where(ahead, now, before).astype(BF16))
            before = now
            if m % 8 == 7 or m == h_blocks:
                k = m // 8
                top = PACK * k
                left = rows - top
                if m < h_blocks:
                    weight = jnp.concatenate(
                        [jnp.concatenate(tiles[i : i + 2], axis=1) for i in range(0, 8, 2)], axis=0
                    )
                    data = jnp.concatenate([even[:left], odd[:left]], axis=1)
                else:
                    weight = jnp.concatenate([tiles[0], jnp.zeros((HALF, LANES), BF16)], axis=0)
                    weight = jnp.concatenate([weight, jnp.zeros((LANES, LANES), BF16)], axis=1)
                    data = even[:left]
                part = jnp.dot(data, weight, preferred_element_type=F32)
                z = part if z is None else jnp.concatenate([z[:top], z[top:] + part], axis=0)
                tiles = []
        zs0[pl.ds(c, rows, stride=pitch), :] = z[:, :LANES]
        zs1[pl.ds(c, rows, stride=pitch), :] = z[:, LANES:]

    def group(g, carry):
        for i in range(each):
            channel(g * each + i)
        return carry

    lax.fori_loop(0, channels // each, group, 0)

    def gather(s, carry):
        late1, late2, late22 = carry
        for b in range(per_source):
            first = pltpu.roll(zs0[place(s, b, 1), :], HALF, 1)
            second = pltpu.roll(zs1[place(s, b, 1), :], HALF, 1)
            y = zs0[place(s, b, 0), :] + jnp.where(low, 0.0, first) + late1 + late22
            late1 = zs1[place(s, b, 0), :] + jnp.where(low, first, second)
            late22, late2 = late2, jnp.where(low, second, 0.0)
            y_ref[s, :, pl.ds(b * LANES, LANES)] = y.astype(BF16)
        return late1, late2, late22

    lax.fori_loop(0, sources, gather, (zero, zero, zero))


def convolve(data, span):
    sources, channels, both = data.shape
    taps = sources * (both - span)
    inputs = [data]
    if (both - span) % LANES:
        inputs.append(jnp.moveaxis(data[:, :, span:], 0, 1).reshape(1, channels, taps))
    blocks = sources * span // LANES
    scratch = [
        pltpu.VMEM((2 * blocks * (channels + 8), LANES), F32),
        pltpu.VMEM((taps // LANES * (channels + 8), LANES), F32),
        pltpu.VMEM((2 * blocks * (channels + 8), LANES), F32),
        pltpu.VMEM((2 * blocks * (channels + 8), LANES), F32),
    ]
    return vmem_call(
        conv_body,
        jax.ShapeDtypeStruct((sources, channels, span), BF16),
        scratch,
        flops=4 * channels * blocks * (taps // 4 + HALF) * WIDE,
        name="conv",
        limit=28,
        inputs=len(inputs),
    )(*inputs)


def mix(k, chunks, has_before, y_ref, gated_ref, og_ref, column_ref, *refs):
    mixed_ref, power_ref = refs[-2:]
    owners, part, tokens = y_ref.shape
    power_ref[...] = refs[0][...] if has_before else jnp.zeros((8, tokens), F32)

    def some(owner, carry):
        at = (owner * chunks + k) * part
        skip = column_ref[pl.ds(at if part % 8 else pl.multiple_of(at, 8), part), :1]
        mixed = og_ref[owner].astype(F32) * (
            y_ref[owner].astype(F32) + skip * gated_ref[owner, :, :tokens].astype(F32)
        )
        mixed_ref[owner] = mixed
        square = mixed * mixed
        if part % 8:
            power_ref[pl.ds(0, 1), :] += jnp.sum(square, axis=0, keepdims=True)
        else:
            power_ref[...] += jnp.sum(square.reshape(part // 8, 8, tokens), axis=0)
        return carry

    lax.fori_loop(0, owners, some, 0)
    power_ref[...] = jnp.broadcast_to(jnp.sum(power_ref[...], axis=0, keepdims=True), (8, tokens))


def finish(total, peers, *refs):
    powers, mixed, (out_hbm, out_ref, sems) = refs[:peers], refs[peers:-3], refs[-3:]
    step = min(WIDE, out_ref.shape[0])
    steps = out_ref.shape[0] // step
    unit = unit_matrix(step)
    owners = mixed[0].shape[0]

    def leave(i):
        rows = pl.ds(i * step if isinstance(i, int) else pl.multiple_of(i * step, step), step)
        return pltpu.make_async_copy(out_ref.at[rows, :], out_hbm.at[rows, :], sems.at[i])

    def some(i, carry):
        rows = pl.ds(pl.multiple_of(i * step, step), step)
        power = powers[0][:1, rows]
        for other in powers[1:]:
            power = power + other[:1, rows]
        scale = 1.0 / jnp.sqrt(power / total + 1e-05)
        pieces = [
            (ref[owner, :, rows] * scale).astype(BF16) for owner in range(owners) for ref in mixed
        ]
        out_ref[rows, :] = flip(jnp.concatenate(pieces, axis=0), unit)
        leave(i).start()
        return carry

    lax.fori_loop(0, steps, some, 0)
    for i in range(steps):
        leave(i).wait()


def local(n_seq, n_mp, gate_in, value_in, out_gate, filter_taps, skip_gain):
    tokens, channels = gate_in.shape
    taps = filter_taps.shape[0]
    share = channels // n_seq
    chunks = CHUNKS if share % (16 * CHUNKS) == 0 else 1
    part = share // chunks
    swap = functools.partial(lax.all_to_all, axis_name="seq", split_axis=0, concat_axis=0, tiled=True)
    dealt = [jax.ShapeDtypeStruct((n_seq, part, tokens), BF16)] * chunks
    dealt_both = [jax.ShapeDtypeStruct((n_seq, part, tokens + taps), BF16)] * chunks
    column = jax.ShapeDtypeStruct((channels, LANES), F32)
    flat = [jax.ShapeDtypeStruct((n_seq, part, tokens), F32), jax.ShapeDtypeStruct((8, tokens), F32)]
    product = 2 * channels * channels
    both = vmem_call(
        flip_in,
        dealt_both,
        [
            pltpu.VMEM((tokens, channels), BF16),
            pltpu.VMEM((tokens, channels), BF16),
            pltpu.VMEM((taps, channels), BF16),
            pltpu.SemaphoreType.DMA((3, max(1, tokens // WIDE))),
        ],
        name="flip_in",
        flops=product * (tokens + taps),
        inputs=3,
        fetch=True,
        limit=60,
    )(gate_in, value_in, filter_taps)
    moved = [swap(piece) for piece in both]
    skip, *og = vmem_call(
        flip_out_gate, [column] + dealt, name="flip_out_gate", flops=product * tokens, inputs=2
    )(out_gate, skip_gain.reshape(1, channels))
    y = [swap(convolve(piece, tokens)) for piece in moved]
    mixed, power = [], None
    for k in range(chunks):
        before = [] if power is None else [power]
        piece, power = vmem_call(
            functools.partial(mix, k, chunks, bool(before)),
            flat,
            name="mix",
            flops=8 * channels * tokens,
            inputs=4 + len(before),
        )(y[k], both[k], og[k], skip, *before)
        mixed.append(piece)
    powers = [power] + [
        lax.ppermute(power[:1], "mp", [(j, (j + d) % n_mp) for j in range(n_mp)])
        for d in range(1, n_mp)
    ]
    return vmem_call(
        functools.partial(finish, channels * n_mp, n_mp),
        jax.ShapeDtypeStruct((tokens, channels), BF16),
        [pltpu.VMEM((tokens, channels), BF16), pltpu.SemaphoreType.DMA((max(1, tokens // WIDE),))],
        name="finish",
        flops=2 * channels * tokens * WIDE,
        inputs=n_mp + chunks,
        store=True,
    )(*powers, *mixed)


def solution(mesh):
    return jax.shard_map(
        functools.partial(local, mesh.shape["seq"], mesh.shape["mp"]),
        mesh=mesh,
        in_specs=(P("seq", "mp"), P("seq", "mp"), P("seq", "mp"), P("seq", "mp"), P("mp")),
        out_specs=P("seq", "mp"),
        check_vma=False,
    )
```

```python
import functools
import math

import jax
import jax.numpy as jnp
from jax import lax
from jax.experimental import pallas as pl
from jax.experimental.pallas import tpu as pltpu
from jax.sharding import PartitionSpec as P

LANES = 128
HALF = LANES // 2
WIDE = 2 * LANES
CHUNKS = 1
BF16 = jnp.bfloat16
F32 = jnp.float32
NT = (((1,), (1,)), ((), ()))


def vmem_call(
    body, out_shape, scratch=(), flops=0, name=None, limit=6, inputs=1, fetch=False, store=False
):
    spec, placed = pl.BlockSpec(memory_space=pltpu.VMEM), pl.BlockSpec(memory_space=pltpu.HBM)
    out_spec = placed if store else spec
    return pl.pallas_call(
        body,
        out_shape=out_shape,
        in_specs=[placed if fetch else spec] * inputs,
        out_specs=[out_spec] * len(out_shape) if isinstance(out_shape, (list, tuple)) else out_spec,
        scratch_shapes=list(scratch),
        compiler_params=pltpu.CompilerParams(vmem_limit_bytes=limit << 20),
        cost_estimate=pl.CostEstimate(flops=flops, bytes_accessed=0, transcendentals=0),
        name=name,
    )


def unit_matrix(size):
    row = lax.broadcasted_iota(jnp.int32, (size, size), 0)
    column = lax.broadcasted_iota(jnp.int32, (size, size), 1)
    return jnp.where(row == column, 1.0, 0.0).astype(BF16)


def flip(matrix, unit):
    return lax.dot_general(unit, matrix, NT, preferred_element_type=F32).astype(BF16)


def deal(flipped, refs, span):
    owners, part, _ = refs[0].shape
    for owner in range(owners):
        for k, ref in enumerate(refs):
            at = (owner * len(refs) + k) * part
            ref[owner, :, span] = flipped[at : at + part, :]


def flip_in(gate_hbm, value_hbm, taps_hbm, out_hbm, gate_ref, value_ref, taps_ref, out_ref, sems):
    tokens, taps = gate_ref.shape[0], taps_ref.shape[0]
    step = min(WIDE, tokens)
    steps = tokens // step

    def part(i):
        return pl.ds(i * step if isinstance(i, int) else pl.multiple_of(i * step, step), step)

    def arrive(source, target, lane, i):
        return pltpu.make_async_copy(source.at[part(i), :], target.at[part(i), :], sems.at[lane, i])

    def leave(span, lane, i):
        return pltpu.make_async_copy(
            out_ref.at[:, :, span], out_hbm.at[:, :, span], sems.at[lane, i]
        )

    rest = pltpu.make_async_copy(taps_hbm, taps_ref, sems.at[3, 0])
    rest.start()
    for i in range(steps):
        arrive(gate_hbm, gate_ref, 0, i).start()
        arrive(value_hbm, value_ref, 1, i).start()
    unit = unit_matrix(gate_ref.shape[1])
    behind = pl.ds(tokens, taps)
    rest.wait()
    deal(flip(taps_ref[...], unit), (out_ref,), behind)
    last = leave(behind, 4, 0)
    last.start()

    def some(i, carry):
        arrive(gate_hbm, gate_ref, 0, i).wait()
        arrive(value_hbm, value_ref, 1, i).wait()
        rows = part(i)
        gated = (gate_ref[rows, :].astype(F32) * value_ref[rows, :].astype(F32)).astype(BF16)
        deal(flip(gated, unit), (out_ref,), rows)
        leave(rows, 2, i).start()
        return carry

    lax.fori_loop(0, steps, some, 0, unroll=UNROLL_IN)
    for i in range(steps):
        leave(part(i), 2, i).wait()
    last.wait()


def flip_out_gate(og_ref, skip_ref, column_ref, *out_refs):
    unit = unit_matrix(og_ref.shape[1])
    step = min(WIDE, og_ref.shape[0])

    def some(i, carry):
        rows = pl.ds(pl.multiple_of(i * step, step), step)
        deal(flip(og_ref[rows, :], unit), out_refs, rows)
        return carry

    lax.fori_loop(0, og_ref.shape[0] // step, some, 0)
    column_ref[...] = jnp.broadcast_to(skip_ref[...], (LANES, skip_ref.shape[1])).T


UNROLL = 8
UNROLL_IN = 1
PACK = 16

def conv_body(*refs):
    x_ref, h_ref = refs[0], refs[-8]
    y_hbm, y_ref, vs, hs, zs0, zs1, sems = refs[-7:]
    sources, channels, span = y_ref.shape
    per_source = span // LANES
    blocks = sources * per_source
    h_sources = h_ref.shape[0]
    h_from = span if h_ref is x_ref else 0
    h_per = (h_ref.shape[2] - h_from) // LANES
    h_blocks = h_sources * h_per
    rows = 2 * blocks
    pitch = channels + 8
    each = math.gcd(UNROLL, channels)
    low = lax.broadcasted_iota(jnp.int32, (channels, LANES), 1) < HALF
    zero = jnp.zeros((channels, LANES), F32)

    def place(s, b, j):
        at = (8 * (per_source * s // 4 + b // 4) + 4 * j + b % 4) * pitch
        return pl.ds(at if pitch % 8 else pl.multiple_of(at, 8), channels)

    def spread(s, carry):
        older, old = carry
        for b in range(per_source):
            x = x_ref[s, :, pl.ds(b * LANES, LANES)].astype(F32)
            turned = pltpu.roll(x, HALF, 1)
            vs[place(s, b, 0), :] = jnp.where(low, x, older[1])
            vs[place(s, b, 1), :] = jnp.where(low, turned, older[0])
            older, old = old, (x, turned)
        return older, old

    lax.fori_loop(0, sources, spread, ((zero, zero), (zero, zero)), unroll=4)

    def spread_taps(s, carry):
        for b in range(h_per):
            at = (s * h_per + b) * pitch
            at = at if pitch % 8 else pl.multiple_of(at, 8)
            hs[pl.ds(at, channels), :] = h_ref[s, :, pl.ds(h_from + b * LANES, LANES)].astype(F32)
        return carry

    lax.fori_loop(0, h_sources, spread_taps, 0)

    lane = lax.broadcasted_iota(jnp.int32, (HALF, LANES), 1)
    row = lax.broadcasted_iota(jnp.int32, (HALF, LANES), 0)
    ahead = lane >= row

    def channel(c):
        v = vs[pl.ds(c, rows, stride=pitch), :]
        even = v.astype(BF16)
        odd = jnp.concatenate([jnp.zeros((8, LANES), F32), v[:-8]], axis=0).astype(BF16)
        before = jnp.zeros((HALF, LANES), F32)
        tiles = []
        z = None
        for m in range(h_blocks + 1):
            if m < h_blocks:
                line = jnp.broadcast_to(hs[pl.ds(m * pitch + c, 1), :], (HALF, LANES))
                now = pltpu.roll(line, 0, 1, stride=1, stride_axis=0)
            else:
                now = jnp.zeros((HALF, LANES), F32)
            tiles.append(jnp.where(ahead, now, before).astype(BF16))
            before = now
            if m % 8 == 7 or m == h_blocks:
                k = m // 8
                top = PACK * k
                left = rows - top
                if m < h_blocks:
                    weight = jnp.concatenate(
                        [jnp.concatenate(tiles[i : i + 2], axis=1) for i in range(0, 8, 2)], axis=0
                    )
                    data = jnp.concatenate([even[:left], odd[:left]], axis=1)
                else:
                    weight = jnp.concatenate([tiles[0], jnp.zeros((HALF, LANES), BF16)], axis=0)
                    weight = jnp.concatenate([weight, jnp.zeros((LANES, LANES), BF16)], axis=1)
                    data = even[:left]
                part = jnp.dot(data, weight, preferred_element_type=F32)
                z = part if z is None else jnp.concatenate([z[:top], z[top:] + part], axis=0)
                tiles = []
        zs0[pl.ds(c, rows, stride=pitch), :] = z[:, :LANES]
        zs1[pl.ds(c, rows, stride=pitch), :] = z[:, LANES:]

    def group(g, carry):
        for i in range(each):
            channel(g * each + i)
        return carry

    lax.fori_loop(0, channels // each, group, 0)

    def leave(s):
        return pltpu.make_async_copy(y_ref.at[s], y_hbm.at[s], sems.at[s])

    def gather(s, carry):
        late1, late2, late22 = carry
        for b in range(per_source):
            first = pltpu.roll(zs0[place(s, b, 1), :], HALF, 1)
            second = pltpu.roll(zs1[place(s, b, 1), :], HALF, 1)
            y = zs0[place(s, b, 0), :] + jnp.where(low, 0.0, first) + late1 + late22
            late1 = zs1[place(s, b, 0), :] + jnp.where(low, first, second)
            late22, late2 = late2, jnp.where(low, second, 0.0)
            y_ref[s, :, pl.ds(b * LANES, LANES)] = y.astype(BF16)
        leave(s).start()
        return late1, late2, late22

    lax.fori_loop(0, sources, gather, (zero, zero, zero), unroll=4)

    def left(s, carry):
        leave(s).wait()
        return carry

    lax.fori_loop(0, sources, left, 0)


def convolve(data, span):
    sources, channels, both = data.shape
    taps = sources * (both - span)
    inputs = [data]
    if (both - span) % LANES:
        inputs.append(jnp.moveaxis(data[:, :, span:], 0, 1).reshape(1, channels, taps))
    blocks = sources * span // LANES
    scratch = [
        pltpu.VMEM((sources, channels, span), BF16),
        pltpu.VMEM((2 * blocks * (channels + 8), LANES), F32),
        pltpu.VMEM((taps // LANES * (channels + 8), LANES), F32),
        pltpu.VMEM((2 * blocks * (channels + 8), LANES), F32),
        pltpu.VMEM((2 * blocks * (channels + 8), LANES), F32),
    ]
    scratch.append(pltpu.SemaphoreType.DMA((sources,)))
    return vmem_call(
        conv_body,
        jax.ShapeDtypeStruct((sources, channels, span), BF16),
        scratch,
        flops=4 * channels * blocks * (taps // 4 + HALF) * WIDE,
        name="conv",
        limit=28,
        inputs=len(inputs),
        store=True,
    )(*inputs)


def mix(k, chunks, has_before, y_ref, gated_ref, og_ref, column_ref, *refs):
    mixed_ref, power_ref = refs[-2:]
    owners, part, tokens = y_ref.shape
    power_ref[...] = refs[0][...] if has_before else jnp.zeros((8, tokens), F32)

    def some(owner, carry):
        at = (owner * chunks + k) * part
        skip = column_ref[pl.ds(at if part % 8 else pl.multiple_of(at, 8), part), :1]
        mixed = og_ref[owner].astype(F32) * (
            y_ref[owner].astype(F32) + skip * gated_ref[owner, :, :tokens].astype(F32)
        )
        mixed_ref[owner] = mixed
        square = mixed * mixed
        if part % 8:
            power_ref[pl.ds(0, 1), :] += jnp.sum(square, axis=0, keepdims=True)
        else:
            power_ref[...] += jnp.sum(square.reshape(part // 8, 8, tokens), axis=0)
        return carry

    lax.fori_loop(0, owners, some, 0)
    power_ref[...] = jnp.broadcast_to(jnp.sum(power_ref[...], axis=0, keepdims=True), (8, tokens))


def finish(total, peers, *refs):
    powers, mixed, (out_hbm, out_ref, sems) = refs[:peers], refs[peers:-3], refs[-3:]
    step = min(WIDE, out_ref.shape[0])
    steps = out_ref.shape[0] // step
    unit = unit_matrix(step)
    owners = mixed[0].shape[0]

    def leave(i):
        rows = pl.ds(i * step if isinstance(i, int) else pl.multiple_of(i * step, step), step)
        return pltpu.make_async_copy(out_ref.at[rows, :], out_hbm.at[rows, :], sems.at[i])

    def some(i, carry):
        rows = pl.ds(pl.multiple_of(i * step, step), step)
        power = powers[0][:1, rows]
        for other in powers[1:]:
            power = power + other[:1, rows]
        scale = 1.0 / jnp.sqrt(power / total + 1e-05)
        pieces = [
            (ref[owner, :, rows] * scale).astype(BF16) for owner in range(owners) for ref in mixed
        ]
        out_ref[rows, :] = flip(jnp.concatenate(pieces, axis=0), unit)
        leave(i).start()
        return carry

    lax.fori_loop(0, steps, some, 0, unroll=4)
    for i in range(steps):
        leave(i).wait()


def partner(j, d, count):
    return (j + d) % count if count & (count - 1) else j ^ d


def local(n_seq, n_mp, gate_in, value_in, out_gate, filter_taps, skip_gain):
    tokens, channels = gate_in.shape
    taps = filter_taps.shape[0]
    share = channels // n_seq
    chunks = CHUNKS if share % (16 * CHUNKS) == 0 else 1
    part = share // chunks
    swap = functools.partial(lax.all_to_all, axis_name="seq", split_axis=0, concat_axis=0, tiled=True)
    dealt = [jax.ShapeDtypeStruct((n_seq, part, tokens), BF16)] * chunks
    dealt_both = [jax.ShapeDtypeStruct((n_seq, part, tokens + taps), BF16)] * chunks
    column = jax.ShapeDtypeStruct((channels, LANES), F32)
    flat = [jax.ShapeDtypeStruct((n_seq, part, tokens), F32), jax.ShapeDtypeStruct((8, tokens), F32)]
    product = 2 * channels * channels
    both = [
        vmem_call(
            flip_in,
            dealt_both[0],
            [
                pltpu.VMEM((tokens, channels), BF16),
                pltpu.VMEM((tokens, channels), BF16),
                pltpu.VMEM((taps, channels), BF16),
                pltpu.VMEM(dealt_both[0].shape, BF16),
                pltpu.SemaphoreType.DMA((5, max(1, tokens // WIDE))),
            ],
            name="flip_in",
            flops=product * (tokens + taps),
            inputs=3,
            fetch=True,
            store=True,
            limit=60,
        )(gate_in, value_in, filter_taps)
    ]
    moved = [swap(piece) for piece in both]
    skip, *og = vmem_call(
        flip_out_gate, [column] + dealt, name="flip_out_gate", flops=product * tokens, inputs=2
    )(out_gate, skip_gain.reshape(1, channels))
    y = [swap(convolve(piece, tokens)) for piece in moved]
    mixed, power = [], None
    for k in range(chunks):
        before = [] if power is None else [power]
        piece, power = vmem_call(
            functools.partial(mix, k, chunks, bool(before)),
            flat,
            name="mix",
            flops=8 * channels * tokens,
            inputs=4 + len(before),
        )(y[k], both[k], og[k], skip, *before)
        mixed.append(piece)
    powers = [power] + [
        lax.ppermute(power[:1], "mp", [(j, partner(j, d, n_mp)) for j in range(n_mp)])
        for d in range(1, n_mp)
    ]
    return vmem_call(
        functools.partial(finish, channels * n_mp, n_mp),
        jax.ShapeDtypeStruct((tokens, channels), BF16),
        [pltpu.VMEM((tokens, channels), BF16), pltpu.SemaphoreType.DMA((max(1, tokens // WIDE),))],
        name="finish",
        flops=2 * channels * tokens * WIDE,
        inputs=n_mp + chunks,
        store=True,
    )(*powers, *mixed)


def solution(mesh):
    return jax.shard_map(
        functools.partial(local, mesh.shape["seq"], mesh.shape["mp"]),
        mesh=mesh,
        in_specs=(P("seq", "mp"), P("seq", "mp"), P("seq", "mp"), P("seq", "mp"), P("mp")),
        out_specs=P("seq", "mp"),
        check_vma=False,
    )
```

```python
import functools
import math

import jax
import jax.numpy as jnp
from jax import lax
from jax.experimental import pallas as pl
from jax.experimental.pallas import tpu as pltpu
from jax.sharding import PartitionSpec as P

LANES = 128
HALF = LANES // 2
WIDE = 2 * LANES
BF16 = jnp.bfloat16
F32 = jnp.float32
NT = (((1,), (1,)), ((), ()))


def vmem_call(
    body, out_shape, scratch=(), flops=0, name=None, limit=6, inputs=1, fetch=False, store=False
):
    spec, placed = pl.BlockSpec(memory_space=pltpu.VMEM), pl.BlockSpec(memory_space=pltpu.HBM)
    out_spec = placed if store else spec
    return pl.pallas_call(
        body,
        out_shape=out_shape,
        in_specs=[placed if fetch else spec] * inputs,
        out_specs=[out_spec] * len(out_shape) if isinstance(out_shape, (list, tuple)) else out_spec,
        scratch_shapes=list(scratch),
        compiler_params=pltpu.CompilerParams(vmem_limit_bytes=limit << 20),
        cost_estimate=pl.CostEstimate(flops=flops, bytes_accessed=0, transcendentals=0),
        name=name,
    )


def unit_matrix(size):
    row = lax.broadcasted_iota(jnp.int32, (size, size), 0)
    column = lax.broadcasted_iota(jnp.int32, (size, size), 1)
    return jnp.where(row == column, 1.0, 0.0).astype(BF16)


def flip(matrix, unit):
    return lax.dot_general(unit, matrix, NT, preferred_element_type=F32).astype(BF16)


def deal(flipped, refs, span):
    owners, part, _ = refs[0].shape
    for owner in range(owners):
        for k, ref in enumerate(refs):
            at = (owner * len(refs) + k) * part
            ref[owner, :, span] = flipped[at : at + part, :]


def flip_in(gate_hbm, value_hbm, taps_hbm, *refs):
    away, (gate_ref, value_ref, taps_ref, out_ref, sems, leave_sems) = refs[:-6], refs[-6:]
    tokens, taps = gate_ref.shape[0], taps_ref.shape[0]
    step = min(WIDE, tokens)
    steps = tokens // step

    def part(i):
        return pl.ds(i * step if isinstance(i, int) else pl.multiple_of(i * step, step), step)

    def arrive(source, target, lane, i):
        return pltpu.make_async_copy(source.at[part(i), :], target.at[part(i), :], sems.at[lane, i])

    def leave(d):
        owner = lax.rem(lax.axis_index("seq") + d, len(away))
        return pltpu.make_async_copy(out_ref.at[owner], away[d], leave_sems.at[d])

    rest = pltpu.make_async_copy(taps_hbm, taps_ref, sems.at[2, 0])
    rest.start()
    for i in range(steps):
        arrive(gate_hbm, gate_ref, 0, i).start()
        arrive(value_hbm, value_ref, 1, i).start()
    unit = unit_matrix(gate_ref.shape[1])
    behind = pl.ds(tokens, taps)
    rest.wait()
    deal(flip(taps_ref[...], unit), (out_ref,), behind)

    def some(i, carry):
        arrive(gate_hbm, gate_ref, 0, i).wait()
        arrive(value_hbm, value_ref, 1, i).wait()
        rows = part(i)
        gated = (gate_ref[rows, :].astype(F32) * value_ref[rows, :].astype(F32)).astype(BF16)
        deal(flip(gated, unit), (out_ref,), rows)
        return carry

    lax.fori_loop(0, steps, some, 0, unroll=UNROLL_IN)
    for d in range(len(away)):
        leave(d).start()
    for d in range(len(away)):
        leave(d).wait()


def flip_out_gate(og_ref, skip_ref, column_ref, *out_refs):
    unit = unit_matrix(og_ref.shape[1])
    step = min(WIDE, og_ref.shape[0])

    def some(i, carry):
        rows = pl.ds(pl.multiple_of(i * step, step), step)
        deal(flip(og_ref[rows, :], unit), out_refs, rows)
        return carry

    lax.fori_loop(0, og_ref.shape[0] // step, some, 0)
    column_ref[...] = jnp.broadcast_to(skip_ref[...], (LANES, skip_ref.shape[1])).T


UNROLL = 8
UNROLL_IN = 1
PACK = 16

def conv_body(tap_refs, *refs):
    vs, hs, zs0, zs1, x_ref, y_ref = refs[-6:]
    count = x_ref.shape[0]
    from_refs, out_refs = refs[:count], refs[count + tap_refs : 2 * count + tap_refs]
    here = lax.axis_index("seq")
    for d, ref in enumerate(from_refs):
        x_ref[lax.rem(here + count - d, count)] = ref[...]
    h_ref = refs[count] if tap_refs else x_ref
    sources, channels, span = y_ref.shape
    per_source = span // LANES
    blocks = sources * per_source
    h_sources = h_ref.shape[0]
    h_from = span if h_ref is x_ref else 0
    h_per = (h_ref.shape[2] - h_from) // LANES
    h_blocks = h_sources * h_per
    rows = 2 * blocks
    pitch = channels + 8
    each = math.gcd(UNROLL, channels)
    low = lax.broadcasted_iota(jnp.int32, (channels, LANES), 1) < HALF
    zero = jnp.zeros((channels, LANES), F32)

    def place(s, b, j):
        at = (8 * (per_source * s // 4 + b // 4) + 4 * j + b % 4) * pitch
        return pl.ds(at if pitch % 8 else pl.multiple_of(at, 8), channels)

    def spread(s, carry):
        older, old = carry
        for b in range(per_source):
            x = x_ref[s, :, pl.ds(b * LANES, LANES)].astype(F32)
            turned = pltpu.roll(x, HALF, 1)
            vs[place(s, b, 0), :] = jnp.where(low, x, older[1])
            vs[place(s, b, 1), :] = jnp.where(low, turned, older[0])
            older, old = old, (x, turned)
        return older, old

    lax.fori_loop(0, sources, spread, ((zero, zero), (zero, zero)), unroll=4)

    def spread_taps(s, carry):
        for b in range(h_per):
            at = (s * h_per + b) * pitch
            at = at if pitch % 8 else pl.multiple_of(at, 8)
            hs[pl.ds(at, channels), :] = h_ref[s, :, pl.ds(h_from + b * LANES, LANES)].astype(F32)
        return carry

    lax.fori_loop(0, h_sources, spread_taps, 0)

    lane = lax.broadcasted_iota(jnp.int32, (HALF, LANES), 1)
    row = lax.broadcasted_iota(jnp.int32, (HALF, LANES), 0)
    ahead = lane >= row

    def channel(c):
        v = vs[pl.ds(c, rows, stride=pitch), :]
        even = v.astype(BF16)
        odd = jnp.concatenate([jnp.zeros((8, LANES), F32), v[:-8]], axis=0).astype(BF16)
        before = jnp.zeros((HALF, LANES), F32)
        tiles = []
        z = None
        for m in range(h_blocks + 1):
            if m < h_blocks:
                line = jnp.broadcast_to(hs[pl.ds(m * pitch + c, 1), :], (HALF, LANES))
                now = pltpu.roll(line, 0, 1, stride=1, stride_axis=0)
            else:
                now = jnp.zeros((HALF, LANES), F32)
            tiles.append(jnp.where(ahead, now, before).astype(BF16))
            before = now
            if m % 8 == 7 or m == h_blocks:
                k = m // 8
                top = PACK * k
                left = rows - top
                if m < h_blocks:
                    weight = jnp.concatenate(
                        [jnp.concatenate(tiles[i : i + 2], axis=1) for i in range(0, 8, 2)], axis=0
                    )
                    data = jnp.concatenate([even[:left], odd[:left]], axis=1)
                else:
                    weight = jnp.concatenate([tiles[0], jnp.zeros((HALF, LANES), BF16)], axis=0)
                    weight = jnp.concatenate([weight, jnp.zeros((LANES, LANES), BF16)], axis=1)
                    data = even[:left]
                part = jnp.dot(data, weight, preferred_element_type=F32)
                z = part if z is None else jnp.concatenate([z[:top], z[top:] + part], axis=0)
                tiles = []
        zs0[pl.ds(c, rows, stride=pitch), :] = z[:, :LANES]
        zs1[pl.ds(c, rows, stride=pitch), :] = z[:, LANES:]

    def group(g, carry):
        for i in range(each):
            channel(g * each + i)
        return carry

    lax.fori_loop(0, channels // each, group, 0)

    def gather(s, carry):
        late1, late2, late22 = carry
        for b in range(per_source):
            first = pltpu.roll(zs0[place(s, b, 1), :], HALF, 1)
            second = pltpu.roll(zs1[place(s, b, 1), :], HALF, 1)
            y = zs0[place(s, b, 0), :] + jnp.where(low, 0.0, first) + late1 + late22
            late1 = zs1[place(s, b, 0), :] + jnp.where(low, first, second)
            late22, late2 = late2, jnp.where(low, second, 0.0)
            y_ref[s, :, pl.ds(b * LANES, LANES)] = y.astype(BF16)
        return late1, late2, late22

    lax.fori_loop(0, sources, gather, (zero, zero, zero), unroll=4)

    for d, ref in enumerate(out_refs):
        ref[...] = y_ref[lax.rem(here + d, count)]


def convolve(data, span):
    sources, (channels, both) = len(data), data[0].shape
    taps = sources * (both - span)
    inputs = list(data)
    if (both - span) % LANES:
        here = lax.axis_index("seq")
        pieces = jnp.stack([piece[:, span:] for piece in data[::-1]])
        pieces = jnp.roll(pieces, here + 1, axis=0)
        inputs.append(jnp.moveaxis(pieces, 0, 1).reshape(1, channels, taps))
    blocks = sources * span // LANES
    pitch = channels + 8
    scratch = [
        pltpu.VMEM((2 * blocks * pitch, LANES), F32),
        pltpu.VMEM((taps // LANES * pitch, LANES), F32),
        pltpu.VMEM((2 * blocks * pitch, LANES), F32),
        pltpu.VMEM((2 * blocks * pitch, LANES), F32),
        pltpu.VMEM((sources, channels, both), BF16),
        pltpu.VMEM((sources, channels, span), BF16),
    ]
    return vmem_call(
        functools.partial(conv_body, len(inputs) - sources),
        [jax.ShapeDtypeStruct((channels, span), BF16)] * sources,
        scratch,
        flops=4 * channels * blocks * (taps // 4 + HALF) * WIDE,
        name="conv",
        limit=28,
        inputs=len(inputs),
    )(*inputs)


def mix(*refs):
    og_ref, column_ref, mixed_ref, power_ref, y_ref, gated_ref = refs[-6:]
    owners, part, tokens = y_ref.shape
    for d in range(owners):
        y_ref[d] = refs[d][...]
        gated_ref[d] = refs[owners + (owners - d) % owners][:, :tokens]
    power_ref[...] = jnp.zeros((8, tokens), F32)
    here = lax.axis_index("seq")

    def some(d, carry):
        owner = lax.rem(here + owners - d, owners)
        at = owner * part
        skip = column_ref[pl.ds(at if part % 8 else pl.multiple_of(at, 8), part), :1]
        mixed = og_ref[owner].astype(F32) * (
            y_ref[d].astype(F32) + skip * gated_ref[d].astype(F32)
        )
        mixed_ref[owner] = mixed
        square = mixed * mixed
        if part % 8:
            power_ref[pl.ds(0, 1), :] += jnp.sum(square, axis=0, keepdims=True)
        else:
            power_ref[...] += jnp.sum(square.reshape(part // 8, 8, tokens), axis=0)
        return carry

    lax.fori_loop(0, owners, some, 0)
    power_ref[...] = jnp.broadcast_to(jnp.sum(power_ref[...], axis=0, keepdims=True), (8, tokens))


def finish(total, peers, *refs):
    powers, mixed, (out_hbm, out_ref, sems) = refs[:peers], refs[peers:-3], refs[-3:]
    step = min(WIDE, out_ref.shape[0])
    steps = out_ref.shape[0] // step
    unit = unit_matrix(step)
    owners = mixed[0].shape[0]

    def leave(i):
        rows = pl.ds(i * step if isinstance(i, int) else pl.multiple_of(i * step, step), step)
        return pltpu.make_async_copy(out_ref.at[rows, :], out_hbm.at[rows, :], sems.at[i])

    def some(i, carry):
        rows = pl.ds(pl.multiple_of(i * step, step), step)
        power = powers[0][:1, rows]
        for other in powers[1:]:
            power = power + other[:1, rows]
        scale = 1.0 / jnp.sqrt(power / total + 1e-05)
        pieces = [
            (ref[owner, :, rows] * scale).astype(BF16) for owner in range(owners) for ref in mixed
        ]
        out_ref[rows, :] = flip(jnp.concatenate(pieces, axis=0), unit)
        leave(i).start()
        return carry

    lax.fori_loop(0, steps, some, 0, unroll=4)
    for i in range(steps):
        leave(i).wait()


def partner(j, d, count):
    return (j + d) % count if count & (count - 1) else j ^ d


def exchange(blocks, count):
    return [blocks[0]] + [
        lax.ppermute(block, "seq", [(j, (j + d) % count) for j in range(count)])
        for d, block in enumerate(blocks[1:], 1)
    ]


def local(n_seq, n_mp, gate_in, value_in, out_gate, filter_taps, skip_gain):
    tokens, channels = gate_in.shape
    taps = filter_taps.shape[0]
    part = channels // n_seq
    product = 2 * channels * channels
    blocks = vmem_call(
        flip_in,
        [jax.ShapeDtypeStruct((part, tokens + taps), BF16)] * n_seq,
        [
            pltpu.VMEM((tokens, channels), BF16),
            pltpu.VMEM((tokens, channels), BF16),
            pltpu.VMEM((taps, channels), BF16),
            pltpu.VMEM((n_seq, part, tokens + taps), BF16),
            pltpu.SemaphoreType.DMA((3, max(1, tokens // WIDE))),
            pltpu.SemaphoreType.DMA((n_seq,)),
        ],
        name="flip_in",
        flops=product * (tokens + taps),
        inputs=3,
        fetch=True,
        store=True,
        limit=60,
    )(gate_in, value_in, filter_taps)
    moved = exchange(blocks, n_seq)
    skip, og = vmem_call(
        flip_out_gate,
        [
            jax.ShapeDtypeStruct((channels, LANES), F32),
            jax.ShapeDtypeStruct((n_seq, part, tokens), BF16),
        ],
        name="flip_out_gate",
        flops=product * tokens,
        inputs=2,
    )(out_gate, skip_gain.reshape(1, channels))
    y = exchange(convolve(moved, tokens), n_seq)
    mixed, power = vmem_call(
        mix,
        [
            jax.ShapeDtypeStruct((n_seq, part, tokens), F32),
            jax.ShapeDtypeStruct((8, tokens), F32),
        ],
        [pltpu.VMEM((n_seq, part, tokens), BF16)] * 2,
        name="mix",
        flops=8 * channels * tokens,
        inputs=2 * n_seq + 2,
        limit=8,
    )(*y, *blocks, og, skip)
    powers = [power] + [
        lax.ppermute(power[:1], "mp", [(j, partner(j, d, n_mp)) for j in range(n_mp)])
        for d in range(1, n_mp)
    ]
    return vmem_call(
        functools.partial(finish, channels * n_mp, n_mp),
        jax.ShapeDtypeStruct((tokens, channels), BF16),
        [pltpu.VMEM((tokens, channels), BF16), pltpu.SemaphoreType.DMA((max(1, tokens // WIDE),))],
        name="finish",
        flops=2 * channels * tokens * WIDE,
        inputs=n_mp + 1,
        store=True,
    )(*powers, mixed)


def solution(mesh):
    return jax.shard_map(
        functools.partial(local, mesh.shape["seq"], mesh.shape["mp"]),
        mesh=mesh,
        in_specs=(P("seq", "mp"), P("seq", "mp"), P("seq", "mp"), P("seq", "mp"), P("mp")),
        out_specs=P("seq", "mp"),
        check_vma=False,
    )
```
